256 devices in a mesh: row: 16 (over z, y_lo), col: 16 (over x, y_hi, core).
Axes of the slice: x: 4, y: 4 (y_hi: 2, y_lo: 2; y = y_hi * 2 + y_lo), z: 8, core: 2. Of those that a mesh axis runs over, the one named last changes fastest.
Arguments:
- matrix: float32 [12288, 12288], P('row', 'col'), may hold values from -30 to 30
- panels: float32 [2, 12288, 256], P(None, ('col', 'row')), may hold values from -0.0546875 to 0.0546875
- factors: float32 [2, 256, 256], replicated, may hold values from -1 to 2, as said below
Outputs:
- reduced: float32 [12288, 12288], P('row', 'col')
The draws below stay inside these ranges and needn't reach their ends.
Inputs may be any that keep to these rules, and one draw needn't show every extreme that they name: Each factors[s] is upper triangular with diagonal entries between 1 and 2.
All inputs are finite; a program needn't handle non-finite values.
Results may differ from the reference program's by a relative error of at most 0.0003.
Values sent between devices are 32-bit elements; how exact they have to be, the bound alone decides.
A program may use at most 64 MiB of HBM per device.

```python
import jax
import jax.numpy as jnp
from jax import lax

PANEL = 256
STEPS = 2
ORDER = 12288


def draw_matrix(key, part):
    first_key = jax.random.fold_in(jax.random.fold_in(key, 11), 0)
    noise = jax.random.truncated_normal(first_key, -5.0, 5.0, (ORDER, ORDER), jnp.float32)
    mirror = (noise + noise.T) * 0.5 ** 0.5
    return mirror


def draw_factors(key, part):
    first_key, second_key = jax.random.split(jax.random.fold_in(key, 23))
    diagonal = jax.random.uniform(first_key, (STEPS, PANEL), jnp.float32, 1.0, 2.0)
    spread = jax.random.truncated_normal(second_key, -4.0, 4.0, (STEPS, PANEL, PANEL), jnp.float32) * (0.5 * PANEL ** (-0.5))
    upper = jnp.triu(spread, 1)
    return upper + diagonal[:, :, None] * jnp.eye(PANEL, dtype=jnp.float32)[None, :, :]


def shard_levels(rng, extent, cuts, low, high):
    def one(position, blocks):
        steps = jax.random.uniform(jax.random.fold_in(jax.random.fold_in(rng, 6), position), (blocks,), jnp.float32, low / len(cuts), high / len(cuts))
        return jnp.repeat(jnp.exp(steps), extent[position] // blocks).reshape((-1,) + (1,) * (len(extent) - position - 1))

    level = one(*cuts[0])
    for cut in cuts[1:]:
        level = level * one(*cut)
    return level


def normal_values(rng, shape, deviation, reach, cuts=(), held_as=jnp.bfloat16):
    gain = shard_levels(rng, shape, cuts, -0.22, 0.18) if cuts else 1.0
    array = jax.random.normal(rng, shape, jnp.float32) * deviation * gain
    return jnp.minimum(jnp.maximum(array, -reach), reach).astype(held_as)


def setup_inputs(seed: int = 0) -> dict:
    key_of = jax.random.split(jax.random.key(seed), 4)
    return {
        "matrix": draw_matrix(jax.random.fold_in(key_of[3], 71), 0),
        "panels": normal_values(key_of[1], (STEPS, ORDER, PANEL), ORDER ** -0.5, 0.0546875, ((1, 256),), jnp.float32),
        "factors": draw_factors(jax.random.fold_in(key_of[3], 71), 0),
    }


highest = lax.Precision.HIGHEST


def matmul(left, right):
    return jnp.dot(left, right, precision=highest, preferred_element_type=jnp.float32)


def reference(matrix, panels, factors):
    current = matrix
    for section in range(panels.shape[0]):
        panel = panels[section]
        factor = factors[section]
        image = matmul(matmul(current, panel), factor)
        inner = matmul(panel.T, image)
        update = image - 0.5 * matmul(panel, matmul(factor.T, inner))
        current = current - matmul(panel, update.T) - matmul(update, panel.T)
    return current
```

```python
import jax
import jax.numpy as jnp
from jax import lax
from jax.experimental import pallas as pl
from jax.experimental.pallas import tpu as pltpu
from jax.sharding import PartitionSpec as P

MESH = pl.DeviceIdType.MESH
HIGH = lax.Precision.HIGH
N = 16
SHARE = 48
B = 256
TILE = N * SHARE
HALF = TILE // 2
SEMS = 420


def nn(left, right):
    return jnp.dot(left, right, precision=HIGH, preferred_element_type=jnp.float32)


def tn(left, right):
    return lax.dot_general(
        left, right, (((0,), (0,)), ((), ())), precision=HIGH, preferred_element_type=jnp.float32
    )


def nt(left, right):
    return lax.dot_general(
        left, right, (((1,), (1,)), ((), ())), precision=HIGH, preferred_element_type=jnp.float32
    )


CHIPS = [(1, 0), (3, 0), (0, 1), (1, 1), (3, 1), (2, 0), (2, 1)]


def kernel(
    a_hbm, panels, f_ref, out_hbm,
    a, vc, vr, yc, yr, yp, d2d, rs, rx, gblk, gx, gall, gmat, mb, mx, mf, tc, sems,
):
    r = lax.axis_index("row")
    c = lax.axis_index("col")
    z, y = r // 2, r % 2
    x, yh, core = c // 4, (c // 2) % 2, c % 2
    chip = c // 2
    mate = (r, c + 1 - 2 * core)
    y_mate = (r + 1 - 2 * y, c)
    used = [0]

    def sem():
        used[0] += 1
        return sems.at[used[0] - 1]

    outgoing = []

    def send(src, dst, device):
        copy = pltpu.make_async_remote_copy(
            src_ref=src, dst_ref=dst, send_sem=sem(), recv_sem=sem(), device_id=device, device_id_type=MESH
        )
        copy.start()
        outgoing.append(copy)
        return copy

    def z_device(step):
        return (((z + step + 8) % 8) * 2 + y, c)

    def row_device(d):
        return ((r + d) % N, c)

    def chip_col(dx, dy):
        return ((x + dx) % 4) * 4 + ((yh + dy) % 2) * 2 + core

    def ring_start(buf):
        flight = {}
        for p in range(2):
            for way in (1, -1):
                flight[way, 1, 0, p] = send(buf.at[r, p], buf.at[r, p], z_device(way))
            flight[0, 0, 1, p] = send(buf.at[r, p], buf.at[r, p], y_mate)
        for p in range(2):
            flight[0, 0, 1, p].wait_recv()
            other = r + 1 - 2 * y
            for way in (1, -1):
                flight[way, 1, 1, p] = send(buf.at[other, p], buf.at[other, p], z_device(way))
        return flight

    def ring_step(buf, flight, k):
        for line in range(2):
            for p in range(2):
                for way in (1, -1):
                    if (way, k, line, p) not in flight:
                        continue
                    flight[way, k, line, p].wait_recv()
                    if k < 3 or (k == 3 and way == (1, -1)[line]):
                        block = ((z - way * k + 8) % 8) * 2 + (y if line == 0 else 1 - y)
                        flight[way, k + 1, line, p] = send(buf.at[block, p], buf.at[block, p], z_device(way))

    def col_start(buf):
        flight = {}
        for dx, dy in CHIPS:
            flight[dx, dy] = send(buf.at[c], buf.at[c], (r, chip_col(dx, dy)))
        flight["mate"] = [send(buf.at[c], buf.at[c], mate)]
        return flight

    def col_finish(buf, flight):
        for dx, dy in CHIPS:
            flight[dx, dy].wait_recv()
            block = chip_col(4 - dx, dy)
            flight["mate"].append(send(buf.at[block], buf.at[block], mate))
        for copy in flight["mate"]:
            copy.wait_recv()

    class Transpose:
        def __init__(self, src, dst):
            recv = sem()
            self.remote = pltpu.make_async_remote_copy(
                src_ref=src, dst_ref=dst, send_sem=sem(), recv_sem=recv, device_id=(c, r), device_id_type=MESH
            )
            self.local = pltpu.make_async_copy(src, dst, recv)

            @pl.when(r != c)
            def _():
                self.remote.start()

            @pl.when(r == c)
            def _():
                self.local.start()

        def wait(self):
            @pl.when(r != c)
            def _():
                self.remote.wait_recv()

            @pl.when(r == c)
            def _():
                self.local.wait()

        def drain(self):
            @pl.when(r != c)
            def _():
                self.remote.wait_send()

    own_panels = pltpu.make_async_copy(panels, vc.at[r], sem())
    own_panels.start()
    tile_in = pltpu.make_async_copy(a_hbm, a, sem())
    tile_in.start()

    barrier = pltpu.get_barrier_semaphore()
    for d in range(1, N):
        pl.semaphore_signal(barrier, inc=1, device_id=row_device(d), device_id_type=MESH)
        pl.semaphore_signal(barrier, inc=1, device_id=(r, (c + d) % N), device_id_type=MESH)

    @pl.when(r != c)
    def _():
        pl.semaphore_signal(barrier, inc=1, device_id=(c, r), device_id_type=MESH)
        pl.semaphore_wait(barrier, 2 * (N - 1) + 1)

    @pl.when(r == c)
    def _():
        pl.semaphore_wait(barrier, 2 * (N - 1))

    own_panels.wait()

    turned = Transpose(vc.at[r], vr.at[r])
    ring = ring_start(vc)
    ring_step(vc, ring, 1)
    turned.wait()
    rows_v = col_start(vr)
    for k in (2, 3, 4):
        ring_step(vc, ring, k)
    tile_in.wait()

    def panel(buf, p, first=0, count=N):
        return buf[first:first + count, p].reshape(count * SHARE, B)

    pair = []
    for h in range(2):
        for p in range(2):
            part = nn(a[h * HALF:(h + 1) * HALF, :], panel(vc, p)).reshape(4, 2, SHARE, B)
            yp[0, 4 * h:4 * h + 4, p] = part[:, 0]
            yp[1, 4 * h:4 * h + 4, p] = part[:, 1]
        pair.append(send(yp.at[1 - core, pl.ds(4 * h, 4)], d2d.at[pl.ds(4 * h, 4)], mate))

    left = vc[:, 0, :, pl.ds(pl.multiple_of((r % 2) * 128, 128), 128)].reshape(TILE, 128)
    right = vc[:, 1, :, pl.ds(pl.multiple_of(((r // 2) % 2) * 128, 128), 128)].reshape(TILE, 128)
    gblk[...] = tn(left, right).reshape(4, 32, 128)

    for h in range(2):
        pair[h].wait_recv()
        rs[4 * h:4 * h + 4] = yp[core, 4 * h:4 * h + 4] + d2d[4 * h:4 * h + 4]
    parts = []
    for i, (dx, dy) in enumerate(CHIPS):
        parts.append(send(rs.at[chip_col(dx, dy) // 2], rx.at[i], (r, chip_col(dx, dy))))
    g_parts = [send(gblk.at[r // 4], gx.at[d], (r, (c + d) % N)) for d in range(1, N)]
    col_finish(vr, rows_v)
    for copy in g_parts:
        copy.wait_recv()
    total = gblk[r // 4]
    for d in range(1, N):
        total += gx[d]
    gall[r] = total
    g_all = [send(gall.at[r], gall.at[r], row_device(d)) for d in range(1, N)]
    for copy in g_all:
        copy.wait_recv()
    for i in range(N):
        bi, bj, s = i % 2, (i // 2) % 2, i // 4
        gmat[128 * bi + 32 * s:128 * bi + 32 * s + 32, 128 * bj:128 * bj + 128] = gall[i]

    f1, f2 = f_ref[0], f_ref[1]
    gf2 = nn(gmat[...], f2)
    for copy in parts:
        copy.wait_recv()
    y1 = rs[chip, 0]
    y2 = rs[chip, 1]
    for i in range(len(CHIPS)):
        y1 += rx[i, 0]
        y2 += rx[i, 1]
    first = nn(y1, f1)
    yr[c, 0] = first
    yr[c, 1] = nn(y2, f2) - nn(first, gf2)

    turned_y = Transpose(yr.at[c], yc.at[c])
    rows_y = col_start(yr)
    turned_y.wait()
    ring = ring_start(yc)
    col_finish(yr, rows_y)

    left = vr[:, (chip // 2 + 2) // 3, :, pl.ds(pl.multiple_of(core * 128, 128), 128)].reshape(TILE, 128)
    right = yr[:, chip // 4, :, pl.ds(pl.multiple_of((chip % 2) * 128, 128), 128)].reshape(TILE, 128)
    mb[...] = tn(left, right).reshape(N, 8, 128)
    m_parts = [send(mb.at[(r + d) % N], mx.at[d], row_device(d)) for d in range(1, N)]
    ring_step(yc, ring, 1)
    for copy in m_parts:
        copy.wait_recv()
    total = mb[r]
    for d in range(1, N):
        total += mx[d]
    mf[c, r] = total
    m_all = [send(mf.at[c, r], mf.at[c, r], row_device(d)) for d in range(1, N)]
    ring_step(yc, ring, 2)
    for copy in m_all:
        copy.wait_recv()
    rows_m = col_start(mf)
    ring_step(yc, ring, 3)
    for h in range(2):
        rows = slice(h * HALF, (h + 1) * HALF)
        a[rows, :] -= nt(panel(yr, 0, 8 * h, 8), panel(vc, 0)) + nt(panel(yr, 1, 8 * h, 8), panel(vc, 1))
    ring_step(yc, ring, 4)
    col_finish(mf, rows_m)

    def block(i):
        def part(q, k):
            return mf[2 * q + k].reshape(128, 128)

        return jnp.concatenate(
            [jnp.concatenate([part(2 * i, k), part(2 * i + 1, k)], axis=1) for k in range(2)], axis=0
        )

    g = gmat[...]
    k1 = tn(f1, block(0))
    h_mat = block(1).T - 0.5 * tn(k1, g)
    l_mat = nn(h_mat - 0.5 * nn(k1, g), f2)
    k2 = tn(f2, block(2) - tn(g, l_mat))
    r11 = -0.5 * (k1 + k1.T)
    r22 = -0.5 * (k2 + k2.T)
    v1, v2 = panel(vc, 0), panel(vc, 1)
    tc[0] = panel(yc, 0) + nn(v1, r11) - nt(v2, l_mat)
    tc[1] = panel(yc, 1) - nn(v1, l_mat) + nn(v2, r22)
    out_copies = []
    for h in range(2):
        rows = slice(h * HALF, (h + 1) * HALF)
        a[rows, :] -= nt(panel(vr, 0, 8 * h, 8), tc[0]) + nt(panel(vr, 1, 8 * h, 8), tc[1])
        copy = pltpu.make_async_copy(a.at[pl.ds(h * HALF, HALF)], out_hbm.at[pl.ds(h * HALF, HALF)], sem())
        copy.start()
        out_copies.append(copy)
    for copy in outgoing:
        copy.wait_send()
    turned.drain()
    turned_y.drain()
    for copy in out_copies:
        copy.wait()
    assert used[0] <= SEMS


def per_device(matrix, panels, factors):
    f32 = jnp.float32
    blocks = pltpu.VMEM((N, 2, SHARE, B), f32)
    return pl.pallas_call(
        kernel,
        out_shape=jax.ShapeDtypeStruct((TILE, TILE), f32),
        in_specs=[
            pl.BlockSpec(memory_space=pl.ANY),
            pl.BlockSpec(memory_space=pl.ANY),
            pl.BlockSpec(memory_space=pltpu.VMEM),
        ],
        out_specs=pl.BlockSpec(memory_space=pl.ANY),
        scratch_shapes=[
            pltpu.VMEM((TILE, TILE), f32),
            blocks,
            blocks,
            blocks,
            blocks,
            pltpu.VMEM((2, 8, 2, SHARE, B), f32),
            pltpu.VMEM((8, 2, SHARE, B), f32),
            pltpu.VMEM((8, 2, SHARE, B), f32),
            pltpu.VMEM((7, 2, SHARE, B), f32),
            pltpu.VMEM((4, 32, 128), f32),
            pltpu.VMEM((N, 32, 128), f32),
            pltpu.VMEM((N, 32, 128), f32),
            pltpu.VMEM((B, B), f32),
            pltpu.VMEM((N, 8, 128), f32),
            pltpu.VMEM((N, 8, 128), f32),
            pltpu.VMEM((N, N, 8, 128), f32),
            pltpu.VMEM((2, TILE, B), f32),
            pltpu.SemaphoreType.DMA((SEMS,)),
        ],
        compiler_params=pltpu.CompilerParams(
            collective_id=0, has_side_effects=True, vmem_limit_bytes=60 * 1024 * 1024
        ),
    )(matrix, panels, factors)


def solution(mesh):
    return jax.shard_map(
        per_device,
        mesh=mesh,
        in_specs=(P("row", "col"), P(None, ("col", "row"), None), P()),
        out_specs=P("row", "col"),
        check_vma=False,
    )
```

```python
import jax
import jax.numpy as jnp
from jax import lax
from jax.experimental import pallas as pl
from jax.experimental.pallas import tpu as pltpu
from jax.sharding import PartitionSpec as P

MESH = pl.DeviceIdType.MESH
HIGH = lax.Precision.HIGH
N = 16
SHARE = 48
B = 256
TILE = N * SHARE
HALF = TILE // 2
SEMS = 540


def nn(left, right):
    return jnp.dot(left, right, precision=HIGH, preferred_element_type=jnp.float32)


def tn(left, right):
    return lax.dot_general(
        left, right, (((0,), (0,)), ((), ())), precision=HIGH, preferred_element_type=jnp.float32
    )


def nt(left, right):
    return lax.dot_general(
        left, right, (((1,), (1,)), ((), ())), precision=HIGH, preferred_element_type=jnp.float32
    )


NEAR = (1, 2)
CHIPS = [(1, 0), (3, 0), (0, 1), (1, 1), (3, 1), (2, 0), (2, 1)]


def kernel(
    a_hbm, panels, f_hbm, out,
    a, vc, vr, yc, yr, yp, d2d, rs, rx, gblk, gx, gall, gmat, ym, yx, mb, mx, mf, tc, f_ref, sems,
):
    r = lax.axis_index("row")
    c = lax.axis_index("col")
    z, y = r // 2, r % 2
    x, yh, core = c // 4, (c // 2) % 2, c % 2
    chip = c // 2
    mate = (r, c + 1 - 2 * core)
    y_mate = (r + 1 - 2 * y, c)
    used = [0]

    def sem():
        used[0] += 1
        return sems.at[used[0] - 1]

    outgoing = []

    def send(src, dst, device):
        copy = pltpu.make_async_remote_copy(
            src_ref=src, dst_ref=dst, send_sem=sem(), recv_sem=sem(), device_id=device, device_id_type=MESH
        )
        copy.start()
        outgoing.append(copy)
        return copy

    def z_device(step):
        return (((z + step + 8) % 8) * 2 + y, c)

    def row_device(d):
        return ((r + d) % N, c)

    def chip_at(dx, dy):
        return ((x + dx) % 4) * 2 + (yh + dy) % 2

    def block_at(way, k, line):
        return ((z - way * k + 8) % 8) * 2 + (y if line == 0 else 1 - y)

    def ring_start(buf, flight, p):
        for way in (1, -1):
            flight[way, 1, 0, p] = send(buf.at[r, p], buf.at[r, p], z_device(way))
        flight[0, p] = send(buf.at[r, p], buf.at[r, p], y_mate)

    def ring_mates(buf, flight, seen):
        other = r + 1 - 2 * y
        for p in range(2):
            flight[0, p].wait_recv()
            for way in (1, -1):
                flight[way, 1, 1, p] = send(buf.at[other, p], buf.at[other, p], z_device(way))
            seen(other, p)

    def ring_step(buf, flight, k, seen):
        for line in range(2):
            for p in range(2):
                for way in (1, -1):
                    if (way, k, line, p) not in flight:
                        continue
                    flight[way, k, line, p].wait_recv()
                    at = block_at(way, k, line)
                    if line:
                        on = k < NEAR[p]
                    else:
                        on = k < 3 or (k == 3 and way == (1, -1)[p])
                    if on:
                        flight[way, k + 1, line, p] = send(buf.at[at, p], buf.at[at, p], z_device(way))
                    if line == 0 and k > NEAR[p]:
                        flight["y", way, k, p] = send(buf.at[at, p], buf.at[at, p], y_mate)
                    seen(at, p)

    def ring_finish(flight, seen):
        for key in flight:
            if key[0] == "y":
                flight[key].wait_recv()
                seen(block_at(key[1], key[2], 1), key[3])

    def unseen(at, p):
        pass

    def col_start(buf, part=None):
        def at(chip_index):
            return buf.at[chip_index, core] if part is None else buf.at[chip_index, core, part]

        flight = [send(at(chip), at(chip), (r, chip_at(dx, dy) * 2 + core)) for dx, dy in CHIPS]
        return at, flight, [send(at(chip), at(chip), mate)]

    def col_forward(state):
        at, flight, mates = state
        for (dx, dy), copy in zip(CHIPS, flight):
            copy.wait_recv()
            source = chip_at(4 - dx, dy)
            mates.append(send(at(source), at(source), mate))

    def col_finish(state):
        for copy in state[2]:
            copy.wait_recv()

    class Transpose:
        def __init__(self, src, dst):
            recv = sem()
            self.remote = pltpu.make_async_remote_copy(
                src_ref=src, dst_ref=dst, send_sem=sem(), recv_sem=recv, device_id=(c, r), device_id_type=MESH
            )
            self.local = pltpu.make_async_copy(src, dst, recv)

            @pl.when(r != c)
            def _():
                self.remote.start()

            @pl.when(r == c)
            def _():
                self.local.start()

        def wait(self):
            @pl.when(r != c)
            def _():
                self.remote.wait_recv()

            @pl.when(r == c)
            def _():
                self.local.wait()

        def drain(self):
            @pl.when(r != c)
            def _():
                self.remote.wait_send()

    def finish():
        for copy in outgoing:
            copy.wait_send()
        for item in turned:
            item.drain()

        @pl.when(r == c)
        def _():
            for copy in handed:
                copy.wait_send()

    own_panels = pltpu.make_async_copy(panels, vc.at[r], sem())
    own_panels.start()
    factors_in = pltpu.make_async_copy(f_hbm, f_ref, sem())
    factors_in.start()
    tile_in = pltpu.make_async_copy(a_hbm, a, sem())
    tile_in.start()

    barrier = pltpu.get_barrier_semaphore()
    for device in [z_device(1), z_device(-1), y_mate] + [(r, (c + d) % N) for d in range(1, N)]:
        pl.semaphore_signal(barrier, inc=1, device_id=device, device_id_type=MESH)
    pl.semaphore_wait(barrier, 3 + N - 1)

    own_panels.wait()

    turned = []
    handed = []
    hand_recv = [sem(), sem()]
    own_rows = [pltpu.make_async_copy(vc.at[r, p], vr.at[chip, core, p], hand_recv[p]) for p in range(2)]

    @pl.when(r == c)
    def _():
        for copy in own_rows:
            copy.start()

    def hand(at, p):
        copy = pltpu.make_async_remote_copy(
            src_ref=vc.at[at, p], dst_ref=vr.at[at // 2, at % 2, p], send_sem=sem(), recv_sem=hand_recv[p],
            device_id=(r, at), device_id_type=MESH,
        )
        handed.append(copy)

        @pl.when(r == c)
        def _():
            copy.start()

    ring = {}
    for p in range(2):
        ring_start(vc, ring, p)
    ring_mates(vc, ring, hand)
    for k in (1, 2, 3, 4):
        ring_step(vc, ring, k, hand)
    ring_finish(ring, hand)
    tile_in.wait()
    factors_in.wait()

    def panel(p):
        return vc[:, p].reshape(TILE, B)

    def row_panel(buf, p, h):
        return buf[4 * h:4 * h + 4, :, p].reshape(HALF, B)

    left = vc[:, 0, :, pl.ds(pl.multiple_of((r % 2) * 128, 128), 128)].reshape(TILE, 128)
    right = vc[:, 1, :, pl.ds(pl.multiple_of(((r // 2) % 2) * 128, 128), 128)].reshape(TILE, 128)
    gblk[...] = tn(left, right).reshape(4, 32, 128)
    g_parts = [send(gblk.at[r // 4], gx.at[d], (r, (c + d) % N)) for d in range(1, N)]

    pair = []
    for p in range(2):
        for h in range(2):
            part = nn(a[h * HALF:(h + 1) * HALF, :], panel(p)).reshape(4, 2, SHARE, B)
            yp[p, 0, 4 * h:4 * h + 4] = part[:, 0]
            yp[p, 1, 4 * h:4 * h + 4] = part[:, 1]
        pair.append(send(yp.at[p, 1 - core], d2d.at[p], mate))
    parts = []
    for p in range(2):
        pair[p].wait_recv()
        rs[p] = yp[p, core] + d2d[p]
        for i, (dx, dy) in enumerate(CHIPS):
            parts.append(send(rs.at[p, chip_at(dx, dy)], rx.at[p, i], (r, chip_at(dx, dy) * 2 + core)))
    for copy in g_parts:
        copy.wait_recv()
    total = gblk[r // 4]
    for d in range(1, N):
        total += gx[d]
    gall[r] = total
    g_all = [send(gall.at[r], gall.at[r], row_device(d)) for d in range(1, N)]
    for copy in own_rows:
        copy.wait()
    rows_v = col_start(vr)
    for copy in g_all:
        copy.wait_recv()
    for i in range(N):
        bi, bj, s = i % 2, (i // 2) % 2, i // 4
        gmat[128 * bi + 32 * s:128 * bi + 32 * s + 32, 128 * bj:128 * bj + 128] = gall[i]
    f1, f2 = f_ref[0], f_ref[1]
    gf2 = nn(gmat[...], f2)

    def summed(p):
        for copy in parts[p * len(CHIPS):(p + 1) * len(CHIPS)]:
            copy.wait_recv()
        total = rs[p, chip]
        for i in range(len(CHIPS)):
            total += rx[p, i]
        return total

    first = nn(summed(0), f1)
    yr[chip, core, 0] = first
    turned_y = [Transpose(yr.at[chip, core, 0], yc.at[c, 0])]
    second = nn(summed(1), f2) - nn(first, gf2)
    yr[chip, core, 1] = second
    turned_y.append(Transpose(yr.at[chip, core, 1], yc.at[c, 1]))
    turned += turned_y
    for w, value in enumerate((first, second)):
        for half in range(2):
            ym[2 * w + half] = value[:, 128 * half:128 * half + 128]

    slices = []
    for dx, dy in CHIPS:
        other = chip_at(dx, dy)
        slices.append(send(ym.at[(other // 4) * 2 + other % 2], yx.at[chip], (r, other * 2 + core)))
    yx[chip] = ym[(chip // 4) * 2 + chip % 2]
    for copy in slices:
        copy.wait_recv()
    col_forward(rows_v)
    left = vr[:, core, (chip // 2 + 2) // 3].reshape(HALF, B)
    mb[...] = tn(left, yx[...].reshape(HALF, 128)).reshape(2, N, 8, 128)
    m_parts = []
    for d in range(N):
        for k in range(2):
            if d or k:
                row, other = (r + d) % N, (core + k) % 2
                m_parts.append(send(mb.at[other, row], mx.at[core, r], (row, chip * 2 + other)))
    mx[core, r] = mb[core, r]
    ring = {}
    for p in range(2):
        turned_y[p].wait()
        ring_start(yc, ring, p)
    rows_y = [col_start(yr, p) for p in range(2)]
    for copy in m_parts:
        copy.wait_recv()
    mf[chip, core, r] = mx[...].reshape(2 * N, 8, 128).sum(axis=0)
    m_all = [send(mf.at[chip, core, r], mf.at[chip, core, r], row_device(d)) for d in range(1, N)]
    ring_mates(yc, ring, unseen)
    ring_step(yc, ring, 1, unseen)
    for copy in m_all:
        copy.wait_recv()
    rows_m = col_start(mf)
    ring_step(yc, ring, 2, unseen)
    for state in rows_y:
        col_forward(state)
    ring_step(yc, ring, 3, unseen)
    col_forward(rows_m)
    ring_step(yc, ring, 4, unseen)
    for state in [rows_v] + rows_y:
        col_finish(state)
    for h in range(2):
        rows = slice(h * HALF, (h + 1) * HALF)
        a[rows, :] -= nt(row_panel(yr, 0, h), panel(0)) + nt(row_panel(yr, 1, h), panel(1))
    col_finish(rows_m)

    def block(i):
        return jnp.concatenate([mf[2 * i].reshape(B, 128), mf[2 * i + 1].reshape(B, 128)], axis=1)

    g = gmat[...]
    k1 = tn(f1, block(0))
    h_mat = block(1).T - 0.5 * tn(k1, g)
    l_mat = nn(h_mat - 0.5 * nn(k1, g), f2)
    k2 = tn(f2, block(2) - tn(g, l_mat))
    r11 = -0.5 * (k1 + k1.T)
    r22 = -0.5 * (k2 + k2.T)
    v1, v2 = panel(0), panel(1)
    tc[0] = nn(v1, r11) - nt(v2, l_mat)
    tc[1] = nn(v2, r22) - nn(v1, l_mat)
    ring_finish(ring, unseen)
    for p in range(2):
        tc[p] += yc[:, p].reshape(TILE, B)
    for h in range(2):
        rows = slice(h * HALF, (h + 1) * HALF)
        out[rows, :] = a[rows, :] - (nt(row_panel(vr, 0, h), tc[0]) + nt(row_panel(vr, 1, h), tc[1]))
    finish()
    assert used[0] <= SEMS


def per_device(matrix, panels, factors):
    f32 = jnp.float32
    blocks = pltpu.VMEM((N, 2, SHARE, B), f32)
    row_blocks = pltpu.VMEM((8, 2, 2, SHARE, B), f32)
    return pl.pallas_call(
        kernel,
        out_shape=jax.ShapeDtypeStruct((TILE, TILE), f32),
        in_specs=[
            pl.BlockSpec(memory_space=pltpu.HBM),
            pl.BlockSpec(memory_space=pltpu.HBM),
            pl.BlockSpec(memory_space=pltpu.HBM),
        ],
        out_specs=pl.BlockSpec(memory_space=pltpu.VMEM),
        scratch_shapes=[
            pltpu.VMEM((TILE, TILE), f32),
            blocks,
            row_blocks,
            blocks,
            row_blocks,
            pltpu.VMEM((2, 2, 8, SHARE, B), f32),
            pltpu.VMEM((2, 8, SHARE, B), f32),
            pltpu.VMEM((2, 8, SHARE, B), f32),
            pltpu.VMEM((2, 7, SHARE, B), f32),
            pltpu.VMEM((4, 32, 128), f32),
            pltpu.VMEM((N, 32, 128), f32),
            pltpu.VMEM((N, 32, 128), f32),
            pltpu.VMEM((B, B), f32),
            pltpu.VMEM((4, SHARE, 128), f32),
            pltpu.VMEM((8, SHARE, 128), f32),
            pltpu.VMEM((2, N, 8, 128), f32),
            pltpu.VMEM((2, N, 8, 128), f32),
            pltpu.VMEM((8, 2, N, 8, 128), f32),
            pltpu.VMEM((2, TILE, B), f32),
            pltpu.VMEM((2, B, B), f32),
            pltpu.SemaphoreType.DMA((SEMS,)),
        ],
        compiler_params=pltpu.CompilerParams(
            collective_id=0, has_side_effects=True, vmem_limit_bytes=32 * 1024 * 1024
        ),
    )(*[pltpu.with_memory_space_constraint(value, pltpu.HBM) for value in (matrix, panels, factors)])


def solution(mesh):
    return jax.shard_map(
        per_device,
        mesh=mesh,
        in_specs=(P("row", "col"), P(None, ("col", "row"), None), P()),
        out_specs=P("row", "col"),
        check_vma=False,
    )
```

```python
import jax
import jax.numpy as jnp
from jax import lax
from jax.experimental import pallas as pl
from jax.experimental.pallas import tpu as pltpu
from jax.sharding import PartitionSpec as P

MESH = pl.DeviceIdType.MESH
HIGH = lax.Precision.HIGH
N = 16
SHARE = 48
B = 256
TILE = N * SHARE
HALF = TILE // 2
SEMS = 540


def nn(left, right):
    return jnp.dot(left, right, precision=HIGH, preferred_element_type=jnp.float32)


def tn(left, right):
    return lax.dot_general(
        left, right, (((0,), (0,)), ((), ())), precision=HIGH, preferred_element_type=jnp.float32
    )


def nt(left, right):
    return lax.dot_general(
        left, right, (((1,), (1,)), ((), ())), precision=HIGH, preferred_element_type=jnp.float32
    )


NEAR = (1, 2)
CHIPS = [(1, 0), (3, 0), (0, 1), (1, 1), (3, 1), (2, 0), (2, 1)]


def kernel(
    a_hbm, panels, f_hbm, out,
    a, vc, vr, yc, yr, yp, d2d, rs, rx, gblk, gx, gall, gmat, ym, yx, mb, mx, mf, tc, f_ref, sems,
):
    r = lax.axis_index("row")
    c = lax.axis_index("col")
    z, y = r // 2, r % 2
    x, yh, core = c // 4, (c // 2) % 2, c % 2
    chip = c // 2
    mate = (r, c + 1 - 2 * core)
    y_mate = (r + 1 - 2 * y, c)
    used = [0]

    def sem():
        used[0] += 1
        return sems.at[used[0] - 1]

    outgoing = []

    def send(src, dst, device):
        copy = pltpu.make_async_remote_copy(
            src_ref=src, dst_ref=dst, send_sem=sem(), recv_sem=sem(), device_id=device, device_id_type=MESH
        )
        copy.start()
        outgoing.append(copy)
        return copy

    def z_device(step):
        return (((z + step + 8) % 8) * 2 + y, c)

    def row_device(d):
        return ((r + d) % N, c)

    def chip_at(dx, dy):
        return ((x + dx) % 4) * 2 + (yh + dy) % 2

    def block_at(way, k, line):
        return ((z - way * k + 8) % 8) * 2 + (y if line == 0 else 1 - y)

    def ring_start(buf, flight, p):
        for way in (1, -1):
            flight[way, 1, 0, p] = send(buf.at[r, p], buf.at[r, p], z_device(way))
        flight[0, p] = send(buf.at[r, p], buf.at[r, p], y_mate)

    def ring_mates(buf, flight, seen):
        other = r + 1 - 2 * y
        for p in range(2):
            flight[0, p].wait_recv()
            for way in (1, -1):
                flight[way, 1, 1, p] = send(buf.at[other, p], buf.at[other, p], z_device(way))
            seen(other, p)

    def ring_step(buf, flight, k, seen):
        for line in range(2):
            for p in range(2):
                for way in (1, -1):
                    if (way, k, line, p) not in flight:
                        continue
                    flight[way, k, line, p].wait_recv()
                    at = block_at(way, k, line)
                    if line:
                        on = k < NEAR[p]
                    else:
                        on = k < 3 or (k == 3 and way == (1, -1)[p])
                    if on:
                        flight[way, k + 1, line, p] = send(buf.at[at, p], buf.at[at, p], z_device(way))
                    if line == 0 and k > NEAR[p]:
                        flight["y", way, k, p] = send(buf.at[at, p], buf.at[at, p], y_mate)
                    seen(at, p)

    def ring_finish(flight, seen):
        for key in flight:
            if key[0] == "y":
                flight[key].wait_recv()
                seen(block_at(key[1], key[2], 1), key[3])

    def unseen(at, p):
        pass

    def col_start(buf, part=None):
        def at(chip_index):
            return buf.at[chip_index, core] if part is None else buf.at[chip_index, core, part]

        flight = [send(at(chip), at(chip), (r, chip_at(dx, dy) * 2 + core)) for dx, dy in CHIPS]
        return at, flight, [send(at(chip), at(chip), mate)]

    def col_forward(state):
        at, flight, mates = state
        for (dx, dy), copy in zip(CHIPS, flight):
            copy.wait_recv()
            source = chip_at(4 - dx, dy)
            mates.append(send(at(source), at(source), mate))

    def col_finish(state):
        for copy in state[2]:
            copy.wait_recv()

    class Transpose:
        def __init__(self, src, dst):
            recv = sem()
            self.remote = pltpu.make_async_remote_copy(
                src_ref=src, dst_ref=dst, send_sem=sem(), recv_sem=recv, device_id=(c, r), device_id_type=MESH
            )
            self.local = pltpu.make_async_copy(src, dst, recv)

            @pl.when(r != c)
            def _():
                self.remote.start()

            @pl.when(r == c)
            def _():
                self.local.start()

        def wait(self):
            @pl.when(r != c)
            def _():
                self.remote.wait_recv()

            @pl.when(r == c)
            def _():
                self.local.wait()

        def drain(self):
            @pl.when(r != c)
            def _():
                self.remote.wait_send()

    def finish():
        for copy in outgoing:
            copy.wait_send()
        for item in turned:
            item.drain()

        @pl.when(r == c)
        def _():
            for copy in handed:
                copy.wait_send()

    own_panels = pltpu.make_async_copy(panels, vc.at[r], sem())
    own_panels.start()
    factors_in = pltpu.make_async_copy(f_hbm, f_ref, sem())
    factors_in.start()
    tile_in = pltpu.make_async_copy(a_hbm, a, sem())
    tile_in.start()

    barrier = pltpu.get_barrier_semaphore()
    for device in [z_device(1), z_device(-1), y_mate] + [(r, (c + d) % N) for d in range(1, N)]:
        pl.semaphore_signal(barrier, inc=1, device_id=device, device_id_type=MESH)
    pl.semaphore_wait(barrier, 3 + N - 1)

    own_panels.wait()

    turned = []
    handed = []
    hand_recv = [sem(), sem()]
    own_rows = [pltpu.make_async_copy(vc.at[r, p], vr.at[chip, core, p], hand_recv[p]) for p in range(2)]

    @pl.when(r == c)
    def _():
        for copy in own_rows:
            copy.start()

    def hand(at, p):
        copy = pltpu.make_async_remote_copy(
            src_ref=vc.at[at, p], dst_ref=vr.at[at // 2, at % 2, p], send_sem=sem(), recv_sem=hand_recv[p],
            device_id=(r, at), device_id_type=MESH,
        )
        handed.append(copy)

        @pl.when(r == c)
        def _():
            copy.start()

    ring = {}
    for p in range(2):
        ring_start(vc, ring, p)
    ring_mates(vc, ring, hand)
    for k in (1, 2, 3, 4):
        ring_step(vc, ring, k, hand)
    ring_finish(ring, hand)
    tile_in.wait()
    factors_in.wait()

    def panel(p):
        return vc[:, p].reshape(TILE, B)

    def row_panel(buf, p, h):
        return buf[4 * h:4 * h + 4, :, p].reshape(HALF, B)

    left = vc[:, 0, :, pl.ds(pl.multiple_of((r % 2) * 128, 128), 128)].reshape(TILE, 128)
    right = vc[:, 1, :, pl.ds(pl.multiple_of(((r // 2) % 2) * 128, 128), 128)].reshape(TILE, 128)
    gblk[...] = tn(left, right).reshape(4, 32, 128)
    g_parts = [send(gblk.at[r // 4], gx.at[d], (r, (c + d) % N)) for d in range(1, N)]

    pair = []
    for p in range(2):
        for h in range(2):
            part = nn(a[h * HALF:(h + 1) * HALF, :], panel(p)).reshape(4, 2, SHARE, B)
            yp[p, 0, 4 * h:4 * h + 4] = part[:, 0]
            yp[p, 1, 4 * h:4 * h + 4] = part[:, 1]
        pair.append(send(yp.at[p, 1 - core], d2d.at[p], mate))
    parts = []
    for p in range(2):
        pair[p].wait_recv()
        rs[p] = yp[p, core] + d2d[p]
        for i, (dx, dy) in enumerate(CHIPS):
            parts.append(send(rs.at[p, chip_at(dx, dy)], rx.at[p, i], (r, chip_at(dx, dy) * 2 + core)))
    for copy in g_parts:
        copy.wait_recv()
    total = gblk[r // 4]
    for d in range(1, N):
        total += gx[d]
    gall[r] = total
    g_all = [send(gall.at[r], gall.at[r], row_device(d)) for d in range(1, N)]
    for copy in own_rows:
        copy.wait()
    rows_v = col_start(vr)
    for copy in g_all:
        copy.wait_recv()
    for i in range(N):
        bi, bj, s = i % 2, (i // 2) % 2, i // 4
        gmat[128 * bi + 32 * s:128 * bi + 32 * s + 32, 128 * bj:128 * bj + 128] = gall[i]
    f1, f2 = f_ref[0], f_ref[1]
    gf2 = nn(gmat[...], f2)

    def summed(p):
        for copy in parts[p * len(CHIPS):(p + 1) * len(CHIPS)]:
            copy.wait_recv()
        total = rs[p, chip]
        for i in range(len(CHIPS)):
            total += rx[p, i]
        return total

    first = nn(summed(0), f1)
    yr[chip, core, 0] = first
    turned_y = [Transpose(yr.at[chip, core, 0], yc.at[c, 0])]
    second = nn(summed(1), f2) - nn(first, gf2)
    yr[chip, core, 1] = second
    turned_y.append(Transpose(yr.at[chip, core, 1], yc.at[c, 1]))
    turned += turned_y
    for w, value in enumerate((first, second)):
        for half in range(2):
            ym[2 * w + half] = value[:, 128 * half:128 * half + 128]

    slices = []
    for dx, dy in CHIPS:
        other = chip_at(dx, dy)
        slices.append(send(ym.at[(other // 4) * 2 + other % 2], yx.at[chip], (r, other * 2 + core)))
    yx[chip] = ym[(chip // 4) * 2 + chip % 2]
    for copy in slices:
        copy.wait_recv()
    col_forward(rows_v)
    left = vr[:, core, (chip // 2 + 2) // 3].reshape(HALF, B)
    mb[...] = tn(left, yx[...].reshape(HALF, 128)).reshape(2, N, 8, 128)
    m_parts = []
    for d in range(N):
        for k in range(2):
            if d or k:
                row, other = (r + d) % N, (core + k) % 2
                m_parts.append(send(mb.at[other, row], mx.at[core, r], (row, chip * 2 + other)))
    mx[core, r] = mb[core, r]
    ring = {}
    for p in range(2):
        turned_y[p].wait()
        ring_start(yc, ring, p)
    rows_y = [col_start(yr, p) for p in range(2)]
    for copy in m_parts:
        copy.wait_recv()
    mf[chip, core, r] = mx[...].reshape(2 * N, 8, 128).sum(axis=0)
    m_all = [send(mf.at[chip, core, r], mf.at[chip, core, r], row_device(d)) for d in range(1, N)]
    ring_mates(yc, ring, unseen)
    ring_step(yc, ring, 1, unseen)
    for copy in m_all:
        copy.wait_recv()
    rows_m = col_start(mf)
    ring_step(yc, ring, 2, unseen)
    for state in rows_y:
        col_forward(state)
    ring_step(yc, ring, 3, unseen)
    for state in [rows_v] + rows_y:
        col_finish(state)
    for h in range(2):
        rows = slice(h * HALF, (h + 1) * HALF)
        a[rows, :] -= nt(row_panel(yr, 0, h), panel(0)) + nt(row_panel(yr, 1, h), panel(1))
    col_forward(rows_m)
    ring_step(yc, ring, 4, unseen)
    col_finish(rows_m)

    def block(i):
        return jnp.concatenate([mf[2 * i].reshape(B, 128), mf[2 * i + 1].reshape(B, 128)], axis=1)

    g = gmat[...]
    k1 = tn(f1, block(0))
    h_mat = block(1).T - 0.5 * tn(k1, g)
    l_mat = nn(h_mat - 0.5 * nn(k1, g), f2)
    k2 = tn(f2, block(2) - tn(g, l_mat))
    r11 = -0.5 * (k1 + k1.T)
    r22 = -0.5 * (k2 + k2.T)
    v1, v2 = panel(0), panel(1)
    tc[0] = nn(v1, r11) - nt(v2, l_mat)
    tc[1] = nn(v2, r22) - nn(v1, l_mat)
    ring_finish(ring, unseen)
    for p in range(2):
        tc[p] += yc[:, p].reshape(TILE, B)
    for h in range(2):
        rows = slice(h * HALF, (h + 1) * HALF)
        out[rows, :] = a[rows, :] - (nt(row_panel(vr, 0, h), tc[0]) + nt(row_panel(vr, 1, h), tc[1]))
    finish()
    assert used[0] <= SEMS


def per_device(matrix, panels, factors):
    f32 = jnp.float32
    blocks = pltpu.VMEM((N, 2, SHARE, B), f32)
    row_blocks = pltpu.VMEM((8, 2, 2, SHARE, B), f32)
    return pl.pallas_call(
        kernel,
        out_shape=jax.ShapeDtypeStruct((TILE, TILE), f32),
        in_specs=[
            pl.BlockSpec(memory_space=pltpu.HBM),
            pl.BlockSpec(memory_space=pltpu.HBM),
            pl.BlockSpec(memory_space=pltpu.HBM),
        ],
        out_specs=pl.BlockSpec(memory_space=pltpu.VMEM),
        scratch_shapes=[
            pltpu.VMEM((TILE, TILE), f32),
            blocks,
            row_blocks,
            blocks,
            row_blocks,
            pltpu.VMEM((2, 2, 8, SHARE, B), f32),
            pltpu.VMEM((2, 8, SHARE, B), f32),
            pltpu.VMEM((2, 8, SHARE, B), f32),
            pltpu.VMEM((2, 7, SHARE, B), f32),
            pltpu.VMEM((4, 32, 128), f32),
            pltpu.VMEM((N, 32, 128), f32),
            pltpu.VMEM((N, 32, 128), f32),
            pltpu.VMEM((B, B), f32),
            pltpu.VMEM((4, SHARE, 128), f32),
            pltpu.VMEM((8, SHARE, 128), f32),
            pltpu.VMEM((2, N, 8, 128), f32),
            pltpu.VMEM((2, N, 8, 128), f32),
            pltpu.VMEM((8, 2, N, 8, 128), f32),
            pltpu.VMEM((2, TILE, B), f32),
            pltpu.VMEM((2, B, B), f32),
            pltpu.SemaphoreType.DMA((SEMS,)),
        ],
        compiler_params=pltpu.CompilerParams(
            collective_id=0, has_side_effects=True, vmem_limit_bytes=32 * 1024 * 1024
        ),
    )(*[pltpu.with_memory_space_constraint(value, pltpu.HBM) for value in (matrix, panels, factors)])


def solution(mesh):
    return jax.shard_map(
        per_device,
        mesh=mesh,
        in_specs=(P("row", "col"), P(None, ("col", "row"), None), P()),
        out_specs=P("row", "col"),
        check_vma=False,
    )
```

```python
import jax
import jax.numpy as jnp
from jax import lax
from jax.experimental import pallas as pl
from jax.experimental.pallas import tpu as pltpu
from jax.sharding import PartitionSpec as P

MESH = pl.DeviceIdType.MESH
HIGH = lax.Precision.HIGH
N = 16
SHARE = 48
B = 256
TILE = N * SHARE
HALF = TILE // 2
SEMS = 540


def nn(left, right):
    return jnp.dot(left, right, precision=HIGH, preferred_element_type=jnp.float32)


def tn(left, right):
    return lax.dot_general(
        left, right, (((0,), (0,)), ((), ())), precision=HIGH, preferred_element_type=jnp.float32
    )


def nt(left, right):
    return lax.dot_general(
        left, right, (((1,), (1,)), ((), ())), precision=HIGH, preferred_element_type=jnp.float32
    )


NEAR = (1, 2)
CHIPS = [(1, 0), (3, 0), (0, 1), (1, 1), (3, 1), (2, 0), (2, 1)]


def kernel(
    a_hbm, panels, f_hbm, out,
    a, vc, vr, yc, yr, yp, d2d, rs, rx, gblk, gx, gall, gmat, ym, yx, mb, mx, mf, tc, f_ref, sems,
):
    r = lax.axis_index("row")
    c = lax.axis_index("col")
    z, y = r // 2, r % 2
    x, yh, core = c // 4, (c // 2) % 2, c % 2
    chip = c // 2
    mate = (r, c + 1 - 2 * core)
    y_mate = (r + 1 - 2 * y, c)
    used = [0]

    def sem():
        used[0] += 1
        return sems.at[used[0] - 1]

    outgoing = []

    def send(src, dst, device):
        copy = pltpu.make_async_remote_copy(
            src_ref=src, dst_ref=dst, send_sem=sem(), recv_sem=sem(), device_id=device, device_id_type=MESH
        )
        copy.start()
        outgoing.append(copy)
        return copy

    def z_device(step):
        return (((z + step + 8) % 8) * 2 + y, c)

    def row_device(d):
        return ((r + d) % N, c)

    def chip_at(dx, dy):
        return ((x + dx) % 4) * 2 + (yh + dy) % 2

    def block_at(way, k, line):
        return ((z - way * k + 8) % 8) * 2 + (y if line == 0 else 1 - y)

    def ring_start(buf, flight, p):
        for way in (1, -1):
            flight[way, 1, 0, p] = send(buf.at[r, p], buf.at[r, p], z_device(way))
        flight[0, p] = send(buf.at[r, p], buf.at[r, p], y_mate)

    def ring_mates(buf, flight, seen):
        other = r + 1 - 2 * y
        for p in range(2):
            flight[0, p].wait_recv()
            for way in (1, -1):
                flight[way, 1, 1, p] = send(buf.at[other, p], buf.at[other, p], z_device(way))
            seen(other, p)

    def ring_step(buf, flight, k, seen):
        for line in range(2):
            for p in range(2):
                for way in (1, -1):
                    if (way, k, line, p) not in flight:
                        continue
                    flight[way, k, line, p].wait_recv()
                    at = block_at(way, k, line)
                    if line:
                        on = k < NEAR[p]
                    else:
                        on = k < 3 or (k == 3 and way == (1, -1)[p])
                    if on:
                        flight[way, k + 1, line, p] = send(buf.at[at, p], buf.at[at, p], z_device(way))
                    if line == 0 and k > NEAR[p]:
                        flight["y", way, k, p] = send(buf.at[at, p], buf.at[at, p], y_mate)
                    seen(at, p)

    def ring_finish(flight, seen):
        for key in flight:
            if key[0] == "y":
                flight[key].wait_recv()
                seen(block_at(key[1], key[2], 1), key[3])

    def unseen(at, p):
        pass

    def col_start(buf, part=None):
        def at(chip_index):
            return buf.at[chip_index, core] if part is None else buf.at[chip_index, core, part]

        flight = [send(at(chip), at(chip), (r, chip_at(dx, dy) * 2 + core)) for dx, dy in CHIPS]
        return at, flight, [send(at(chip), at(chip), mate)]

    def col_forward(state):
        at, flight, mates = state
        for (dx, dy), copy in zip(CHIPS, flight):
            copy.wait_recv()
            source = chip_at(4 - dx, dy)
            mates.append(send(at(source), at(source), mate))

    def col_finish(state):
        for copy in state[2]:
            copy.wait_recv()

    class Transpose:
        def __init__(self, src, dst):
            recv = sem()
            self.remote = pltpu.make_async_remote_copy(
                src_ref=src, dst_ref=dst, send_sem=sem(), recv_sem=recv, device_id=(c, r), device_id_type=MESH
            )
            self.local = pltpu.make_async_copy(src, dst, recv)

            @pl.when(r != c)
            def _():
                self.remote.start()

            @pl.when(r == c)
            def _():
                self.local.start()

        def wait(self):
            @pl.when(r != c)
            def _():
                self.remote.wait_recv()

            @pl.when(r == c)
            def _():
                self.local.wait()

        def drain(self):
            @pl.when(r != c)
            def _():
                self.remote.wait_send()

    def finish():
        for copy in outgoing:
            copy.wait_send()
        for item in turned:
            item.drain()

        @pl.when(r == c)
        def _():
            for copy in handed:
                copy.wait_send()

    own_panels = pltpu.make_async_copy(panels, vc.at[r], sem())
    own_panels.start()
    factors_in = pltpu.make_async_copy(f_hbm, f_ref, sem())
    factors_in.start()
    tile_in = pltpu.make_async_copy(a_hbm, a, sem())
    tile_in.start()

    barrier = pltpu.get_barrier_semaphore()
    for device in [z_device(1), z_device(-1), y_mate] + [(r, (c + d) % N) for d in range(1, N)]:
        pl.semaphore_signal(barrier, inc=1, device_id=device, device_id_type=MESH)
    pl.semaphore_wait(barrier, 3 + N - 1)

    own_panels.wait()

    turned = []
    handed = []
    hand_recv = [sem(), sem()]
    own_rows = [pltpu.make_async_copy(vc.at[r, p], vr.at[chip, core, p], hand_recv[p]) for p in range(2)]

    @pl.when(r == c)
    def _():
        for copy in own_rows:
            copy.start()

    def hand(at, p):
        copy = pltpu.make_async_remote_copy(
            src_ref=vc.at[at, p], dst_ref=vr.at[at // 2, at % 2, p], send_sem=sem(), recv_sem=hand_recv[p],
            device_id=(r, at), device_id_type=MESH,
        )
        handed.append(copy)

        @pl.when(r == c)
        def _():
            copy.start()

    ring = {}
    for p in range(2):
        ring_start(vc, ring, p)
    ring_mates(vc, ring, hand)
    for k in (1, 2, 3, 4):
        ring_step(vc, ring, k, hand)
    ring_finish(ring, hand)
    tile_in.wait()
    factors_in.wait()

    def panel(p):
        return vc[:, p].reshape(TILE, B)

    def row_panel(buf, p, h):
        return buf[4 * h:4 * h + 4, :, p].reshape(HALF, B)

    left = vc[:, 0, :, pl.ds(pl.multiple_of((r % 2) * 128, 128), 128)].reshape(TILE, 128)
    right = vc[:, 1, :, pl.ds(pl.multiple_of(((r // 2) % 2) * 128, 128), 128)].reshape(TILE, 128)
    gblk[...] = tn(left, right).reshape(4, 32, 128)
    g_parts = [send(gblk.at[r // 4], gx.at[d], (r, (c + d) % N)) for d in range(1, N)]

    pair = []
    for p in range(2):
        for h in range(2):
            part = nn(a[h * HALF:(h + 1) * HALF, :], panel(p)).reshape(4, 2, SHARE, B)
            yp[p, 0, 4 * h:4 * h + 4] = part[:, 0]
            yp[p, 1, 4 * h:4 * h + 4] = part[:, 1]
        pair.append(send(yp.at[p, 1 - core], d2d.at[p], mate))
    parts = []
    for p in range(2):
        pair[p].wait_recv()
        rs[p] = yp[p, core] + d2d[p]
        for i, (dx, dy) in enumerate(CHIPS):
            parts.append(send(rs.at[p, chip_at(dx, dy)], rx.at[p, i], (r, chip_at(dx, dy) * 2 + core)))
    for copy in g_parts:
        copy.wait_recv()
    total = gblk[r // 4]
    for d in range(1, N):
        total += gx[d]
    gall[r] = total
    g_all = [send(gall.at[r], gall.at[r], row_device(d)) for d in range(1, N)]
    for copy in own_rows:
        copy.wait()
    rows_v = col_start(vr)
    f1, f2 = f_ref[0], f_ref[1]

    def summed(p):
        for copy in parts[p * len(CHIPS):(p + 1) * len(CHIPS)]:
            copy.wait_recv()
        total = rs[p, chip]
        for i in range(len(CHIPS)):
            total += rx[p, i]
        return total

    first = nn(summed(0), f1)
    yr[chip, core, 0] = first
    turned_y = [Transpose(yr.at[chip, core, 0], yc.at[c, 0])]
    for copy in g_all:
        copy.wait_recv()
    for i in range(N):
        bi, bj, s = i % 2, (i // 2) % 2, i // 4
        gmat[128 * bi + 32 * s:128 * bi + 32 * s + 32, 128 * bj:128 * bj + 128] = gall[i]
    gf2 = nn(gmat[...], f2)
    second = nn(summed(1), f2) - nn(first, gf2)
    yr[chip, core, 1] = second
    turned_y.append(Transpose(yr.at[chip, core, 1], yc.at[c, 1]))
    turned += turned_y
    for w, value in enumerate((first, second)):
        for half in range(2):
            ym[2 * w + half] = value[:, 128 * half:128 * half + 128]

    slices = []
    for dx, dy in CHIPS:
        other = chip_at(dx, dy)
        slices.append(send(ym.at[(other // 4) * 2 + other % 2], yx.at[chip], (r, other * 2 + core)))
    yx[chip] = ym[(chip // 4) * 2 + chip % 2]
    for copy in slices:
        copy.wait_recv()
    col_forward(rows_v)
    left = vr[:, core, (chip // 2 + 2) // 3].reshape(HALF, B)
    mb[...] = tn(left, yx[...].reshape(HALF, 128)).reshape(2, N, 8, 128)
    m_parts = []
    for d in range(N):
        for k in range(2):
            if d or k:
                row, other = (r + d) % N, (core + k) % 2
                m_parts.append(send(mb.at[other, row], mx.at[core, r], (row, chip * 2 + other)))
    mx[core, r] = mb[core, r]
    ring = {}
    for p in range(2):
        turned_y[p].wait()
        ring_start(yc, ring, p)
    rows_y = [col_start(yr, p) for p in range(2)]
    for copy in m_parts:
        copy.wait_recv()
    mf[chip, core, r] = mx[...].reshape(2 * N, 8, 128).sum(axis=0)
    m_all = [send(mf.at[chip, core, r], mf.at[chip, core, r], row_device(d)) for d in range(1, N)]
    ring_mates(yc, ring, unseen)
    ring_step(yc, ring, 1, unseen)
    for copy in m_all:
        copy.wait_recv()
    rows_m = col_start(mf)
    ring_step(yc, ring, 2, unseen)
    for state in rows_y:
        col_forward(state)
    ring_step(yc, ring, 3, unseen)
    for state in [rows_v] + rows_y:
        col_finish(state)
    for h in range(2):
        rows = slice(h * HALF, (h + 1) * HALF)
        a[rows, :] -= nt(row_panel(yr, 0, h), panel(0)) + nt(row_panel(yr, 1, h), panel(1))
    col_forward(rows_m)
    ring_step(yc, ring, 4, unseen)
    col_finish(rows_m)

    def block(i):
        return jnp.concatenate([mf[2 * i].reshape(B, 128), mf[2 * i + 1].reshape(B, 128)], axis=1)

    g = gmat[...]
    k1 = tn(f1, block(0))
    h_mat = block(1).T - 0.5 * tn(k1, g)
    l_mat = nn(h_mat - 0.5 * nn(k1, g), f2)
    k2 = tn(f2, block(2) - tn(g, l_mat))
    r11 = -0.5 * (k1 + k1.T)
    r22 = -0.5 * (k2 + k2.T)
    v1, v2 = panel(0), panel(1)
    tc[0] = nn(v1, r11) - nt(v2, l_mat)
    tc[1] = nn(v2, r22) - nn(v1, l_mat)
    ring_finish(ring, unseen)
    for p in range(2):
        tc[p] += yc[:, p].reshape(TILE, B)
    for h in range(2):
        rows = slice(h * HALF, (h + 1) * HALF)
        out[rows, :] = a[rows, :] - (nt(row_panel(vr, 0, h), tc[0]) + nt(row_panel(vr, 1, h), tc[1]))
    finish()
    assert used[0] <= SEMS


def per_device(matrix, panels, factors):
    f32 = jnp.float32
    blocks = pltpu.VMEM((N, 2, SHARE, B), f32)
    row_blocks = pltpu.VMEM((8, 2, 2, SHARE, B), f32)
    return pl.pallas_call(
        kernel,
        out_shape=jax.ShapeDtypeStruct((TILE, TILE), f32),
        in_specs=[
            pl.BlockSpec(memory_space=pltpu.HBM),
            pl.BlockSpec(memory_space=pltpu.HBM),
            pl.BlockSpec(memory_space=pltpu.HBM),
        ],
        out_specs=pl.BlockSpec(memory_space=pltpu.VMEM),
        scratch_shapes=[
            pltpu.VMEM((TILE, TILE), f32),
            blocks,
            row_blocks,
            blocks,
            row_blocks,
            pltpu.VMEM((2, 2, 8, SHARE, B), f32),
            pltpu.VMEM((2, 8, SHARE, B), f32),
            pltpu.VMEM((2, 8, SHARE, B), f32),
            pltpu.VMEM((2, 7, SHARE, B), f32),
            pltpu.VMEM((4, 32, 128), f32),
            pltpu.VMEM((N, 32, 128), f32),
            pltpu.VMEM((N, 32, 128), f32),
            pltpu.VMEM((B, B), f32),
            pltpu.VMEM((4, SHARE, 128), f32),
            pltpu.VMEM((8, SHARE, 128), f32),
            pltpu.VMEM((2, N, 8, 128), f32),
            pltpu.VMEM((2, N, 8, 128), f32),
            pltpu.VMEM((8, 2, N, 8, 128), f32),
            pltpu.VMEM((2, TILE, B), f32),
            pltpu.VMEM((2, B, B), f32),
            pltpu.SemaphoreType.DMA((SEMS,)),
        ],
        compiler_params=pltpu.CompilerParams(
            collective_id=0, has_side_effects=True, vmem_limit_bytes=32 * 1024 * 1024
        ),
    )(*[pltpu.with_memory_space_constraint(value, pltpu.HBM) for value in (matrix, panels, factors)])


def solution(mesh):
    return jax.shard_map(
        per_device,
        mesh=mesh,
        in_specs=(P("row", "col"), P(None, ("col", "row"), None), P()),
        out_specs=P("row", "col"),
        check_vma=False,
    )
```
